32 devices in a mesh: heads: 4 (over x, core), ctx: 8 (over z, y).
Axes of the slice: x: 2, y: 2, z: 4, core: 2. Of those that a mesh axis runs over, the one named last changes fastest.
Arguments:
- queries: bfloat16 [1536, 2048], P('ctx', 'heads'), may hold values from -6 to 6
- key_states: bfloat16 [1536, 512], P('ctx', 'heads'), may hold values from -6 to 6
- value_states: bfloat16 [1536, 512], P('ctx', 'heads'), may hold values from -6 to 6
- attention_out: bfloat16 [1536, 2048], P('ctx', 'heads'), may hold values from -2 to 2
- out_grad: bfloat16 [1536, 2048], P('ctx', 'heads'), may hold values from -6 to 6
- log_sum_exp: float32 [16, 1536], P('heads', 'ctx'), may hold values from 0 to 16, as said below
- block_counts: int32 [8], replicated, may hold values from 1 to 3, as said below
- w_query: bfloat16 [4096, 2048], P(None, 'heads'), may hold values from -0.09375 to 0.09375
- w_key: bfloat16 [4096, 512], P(None, 'heads'), may hold values from -0.09375 to 0.09375
- w_value: bfloat16 [4096, 512], P(None, 'heads'), may hold values from -0.09375 to 0.09375
Outputs:
- input_grad: bfloat16 [1536, 4096], P('ctx', 'heads')
- key_grad: float32 [1536, 512], P('ctx', 'heads')
- value_grad: float32 [1536, 512], P('ctx', 'heads')
The draws below stay inside these ranges and needn't reach their ends.
Inputs may be any that keep to these rules, and one draw needn't show every extreme that they name: `block_counts`: one entry equals 3. `log_sum_exp`: finite offsets of each row's scores.
All inputs are finite; a program needn't handle non-finite values.
Results may differ from the reference program's by a relative error of at most 0.0063.
Values may be sent and summed in bfloat16 or wider, within the bound.
No kernel may reach another device: no remote copies, remote signals or barrier semaphores. Data moves between devices by JAX's collectives and lax.ppermute only.
A program may use at most 128 MiB of HBM per device.

```python
import math
import jax
import jax.numpy as jnp
from jax import lax

D_MODEL = 4096
HEAD_DIM = 128
GROUP = 4
CAP = 192
BLOCK = 64
KV_HEADS = 4
TOKENS_CAP = 1536
N_CTX = 8


def shared_counts(key):
    count_key = jax.random.fold_in(key, 101)
    pick_key = jax.random.fold_in(key, 202)
    counts = jax.random.randint(count_key, (N_CTX,), 1, CAP // BLOCK + 1, dtype=jnp.int32)
    chosen = jax.random.randint(pick_key, (), 0, N_CTX, dtype=jnp.int32)
    return jnp.where(jnp.arange(N_CTX, dtype=jnp.int32) == chosen, CAP // BLOCK, counts).astype(jnp.int32)


def draw_block_counts(key, part):
    return shared_counts(key)


def draw_log_sum_exp(key, part):
    counts = shared_counts(key)
    lengths = counts * BLOCK
    offsets = jnp.cumsum(lengths) - lengths
    row_index = jnp.arange(CAP * N_CTX, dtype=jnp.int32)
    device = row_index // CAP
    within = row_index - device * CAP
    position = offsets[device] + within
    visible_keys = (position + 1).astype(jnp.float32)
    noise_key = jax.random.fold_in(key, 303)
    base = jax.random.uniform(noise_key, (KV_HEADS * GROUP, CAP * N_CTX), jnp.float32, 0.3, 1.2)
    return jnp.log(visible_keys)[None, :] + base


def steps_of(rng, shape, split, least, high):
    level = 1.0
    for dim, blocks in split:
        steps = jax.random.uniform(jax.random.fold_in(jax.random.fold_in(rng, 6), dim), (blocks,), jnp.float32, least / len(split), high / len(split))
        level = level * jnp.repeat(jnp.exp(steps), shape[dim] // blocks).reshape((-1,) + (1,) * (len(shape) - 1 - dim))
    return level


def bell_draw(rng, shape, spread, reach, pieces=(), held_as=jnp.bfloat16):
    entries = jax.random.normal(rng, shape, jnp.float32) * spread
    if len(pieces) > 0:
        entries = steps_of(rng, shape, pieces, -0.22, 0.18) * entries
    return jnp.clip(entries, min=-reach, max=reach).astype(held_as)


def setup_inputs(seed: int = 0) -> dict:
    splits = jax.random.split(jax.random.key(seed), 11)
    queries = bell_draw(splits[0], (TOKENS_CAP, KV_HEADS * GROUP * HEAD_DIM), 1.0, 6.0, ((0, 8), (1, 4)))
    key_states = bell_draw(splits[1], (TOKENS_CAP, KV_HEADS * HEAD_DIM), 1.0, 6.0, ((0, 8), (1, 4)))
    value_states = bell_draw(splits[2], (TOKENS_CAP, KV_HEADS * HEAD_DIM), 1.0, 6.0, ((0, 8), (1, 4)))
    attention_out = bell_draw(splits[3], (TOKENS_CAP, KV_HEADS * GROUP * HEAD_DIM), 0.3, 2.0, ((0, 8), (1, 4)))
    out_grad = bell_draw(splits[4], (TOKENS_CAP, KV_HEADS * GROUP * HEAD_DIM), 1.0, 6.0, ((0, 8), (1, 4)))
    log_sum_exp = draw_log_sum_exp(jax.random.fold_in(splits[10], 71), 0)
    block_counts = draw_block_counts(jax.random.fold_in(splits[10], 71), 0)
    w_query = bell_draw(splits[7], (D_MODEL, KV_HEADS * GROUP * HEAD_DIM), D_MODEL ** -0.5, 0.09375, ((1, 4),))
    w_key = bell_draw(splits[8], (D_MODEL, KV_HEADS * HEAD_DIM), D_MODEL ** -0.5, 0.09375, ((1, 4),))
    w_value = bell_draw(splits[9], (D_MODEL, KV_HEADS * HEAD_DIM), D_MODEL ** -0.5, 0.09375, ((1, 4),))
    return dict(queries=queries, key_states=key_states, value_states=value_states, attention_out=attention_out, out_grad=out_grad, log_sum_exp=log_sum_exp, block_counts=block_counts, w_query=w_query, w_key=w_key, w_value=w_value)


def slot_table(block_counts):
    lengths = (block_counts * BLOCK).astype(jnp.int32)
    offsets = (jnp.cumsum(lengths) - lengths).astype(jnp.int32)
    row_index = jnp.arange(CAP * N_CTX, dtype=jnp.int32)
    device = row_index // CAP
    within = row_index - device * CAP
    position = offsets[device] + within
    live = within < lengths[device]
    return (position, live)

def reference(queries, key_states, value_states, attention_out, out_grad, log_sum_exp, block_counts, w_query, w_key, w_value):
    total_rows = CAP * N_CTX
    score_scale = 1.0 / math.sqrt(HEAD_DIM)
    position, live = slot_table(block_counts)
    query_block = math.gcd(total_rows, 512)
    width = GROUP * HEAD_DIM
    query_parts = []
    key_parts = []
    value_parts = []
    for head_num in range(KV_HEADS):
        query_h = queries[:, head_num * width:(head_num + 1) * width].reshape(total_rows, GROUP, HEAD_DIM)
        grad_h = out_grad[:, head_num * width:(head_num + 1) * width].reshape(total_rows, GROUP, HEAD_DIM)
        output_h = attention_out[:, head_num * width:(head_num + 1) * width].reshape(total_rows, GROUP, HEAD_DIM)
        key_h = key_states[:, head_num * HEAD_DIM:(head_num + 1) * HEAD_DIM].astype(jnp.float32)
        value_h = value_states[:, head_num * HEAD_DIM:(head_num + 1) * HEAD_DIM].astype(jnp.float32)
        norm_h = log_sum_exp[head_num * GROUP:(head_num + 1) * GROUP]
        delta_h = lax.optimization_barrier(jnp.sum(grad_h.astype(jnp.float32) * output_h.astype(jnp.float32), axis=2))

        def step_block(totals, block_num):
            key_acc, value_acc = totals
            begin_row = (block_num * query_block).astype(jnp.int32)
            query_blk = lax.dynamic_slice_in_dim(query_h, begin_row, query_block, 0).astype(jnp.float32)
            grad_blk = lax.dynamic_slice_in_dim(grad_h, begin_row, query_block, 0).astype(jnp.float32)
            norm_blk = lax.dynamic_slice_in_dim(norm_h, begin_row, query_block, 1)
            delta_blk = lax.dynamic_slice_in_dim(delta_h, begin_row, query_block, 0)
            query_pos = lax.dynamic_slice_in_dim(position, begin_row, query_block, 0)
            query_live = lax.dynamic_slice_in_dim(live, begin_row, query_block, 0)
            scores = jnp.einsum('qgd,kd->gqk', query_blk, key_h) * score_scale
            visible = query_live[:, None] & live[None, :] & (position[None, :] <= query_pos[:, None])
            probability = jnp.where(visible[None], jnp.exp(scores - norm_blk[:, :, None]), 0.0)
            prob_grad = jnp.einsum('qgd,kd->gqk', grad_blk, value_h)
            score_grad = probability * (prob_grad - delta_blk.T[:, :, None])
            prob_b = probability.astype(jnp.bfloat16).astype(jnp.float32)
            grad_b = score_grad.astype(jnp.bfloat16).astype(jnp.float32)
            query_terms = score_scale * jnp.einsum('gqk,kd->qgd', grad_b, key_h)
            key_acc = key_acc + score_scale * jnp.einsum('gqk,qgd->kd', grad_b, query_blk)
            value_acc = value_acc + jnp.einsum('gqk,qgd->kd', prob_b, grad_blk)
            return ((key_acc, value_acc), query_terms)
        zero_keys = jnp.zeros((total_rows, HEAD_DIM), jnp.float32)
        (key_acc, value_acc), grad_blocks = lax.scan(step_block, (zero_keys, zero_keys), jnp.arange(total_rows // query_block, dtype=jnp.int32))
        query_parts.append(grad_blocks.reshape(total_rows, width))
        key_parts.append(key_acc)
        value_parts.append(value_acc)
    query_grad = jnp.concatenate(query_parts, axis=1)
    key_grad = jnp.concatenate(key_parts, axis=1)
    value_grad = jnp.concatenate(value_parts, axis=1)
    input_grad = jnp.dot(query_grad.astype(jnp.bfloat16), w_query.T, preferred_element_type=jnp.float32)
    input_grad = input_grad + jnp.dot(key_grad.astype(jnp.bfloat16), w_key.T, preferred_element_type=jnp.float32)
    input_grad = input_grad + jnp.dot(value_grad.astype(jnp.bfloat16), w_value.T, preferred_element_type=jnp.float32)
    return (input_grad.astype(jnp.bfloat16), key_grad, value_grad)
```

```python
import functools
import math

import jax
import jax.numpy as jnp
from jax import lax
from jax.experimental import pallas as pl
from jax.experimental.pallas import tpu as pltpu
from jax.sharding import PartitionSpec as P

BLOCK = 64
LOG2E = 1.4426950408889634
FAR = 1e30
LANES = 256


NT = (((1,), (1,)), ((), ()))
NN = (((1,), (0,)), ((), ()))
VMEM = pl.BlockSpec(memory_space=pltpu.VMEM)
SMEM = pl.BlockSpec(memory_space=pltpu.SMEM)


def mm(a, b, dims):
    return lax.dot_general(a, b, dims, preferred_element_type=jnp.float32)


def kernel_call(body, outs, ins, name):
    return pl.pallas_call(
        body,
        out_shape=outs,
        in_specs=[SMEM if kind == "s" else VMEM for kind in ins],
        out_specs=jax.tree.map(lambda _: VMEM, outs),
        name=name,
    )


def stack_heads(ref, group, dim):
    return jnp.concatenate([ref[:, h * dim : (h + 1) * dim] for h in range(group)], axis=0)


def stats_body(group, dim, counts, index, grad, out, norm, stats):
    cap = grad.shape[0]
    live = counts[index[0]] * BLOCK
    cols = []
    ones = jnp.ones((8, dim), jnp.float32)
    lane = lax.broadcasted_iota(jnp.int32, (1, cap), 1)
    for h in range(group):
        cols_h = slice(h * dim, (h + 1) * dim)
        prod = grad[:, cols_h].astype(jnp.float32) * out[:, cols_h].astype(jnp.float32)
        delta = lax.dot_general(
            ones, prod, NT, precision=lax.Precision.HIGHEST, preferred_element_type=jnp.float32
        )[0:1]
        norm_h = jnp.where(lane < live, norm[h : h + 1, :] * LOG2E, FAR)
        cols.append((norm_h, delta))
    stats[0:1, :] = jnp.concatenate([c[0] for c in cols], axis=1)
    stats[1:2, :] = jnp.concatenate([c[1] for c in cols], axis=1)


def masked_keys(kv, dim, live):
    rows = lax.broadcasted_iota(jnp.int32, (kv.shape[0], dim), 0)
    keys = jnp.where(rows < live, kv[:, :dim].astype(jnp.float32), 0.0)
    return keys.astype(jnp.bfloat16), keys.T.astype(jnp.bfloat16)


def score_terms(keys, keys_t, values, query, grad, norm, delta, mask):
    scale = LOG2E / math.sqrt(query.shape[1])
    prob = jnp.exp2(mm(keys, query, NT) * scale - norm)
    if mask is not None:
        prob = jnp.where(mask, prob, 0.0)
    score_grad = prob * (mm(values, grad, NT) - delta)
    prob_b = prob.astype(jnp.bfloat16)
    grad_b = score_grad.astype(jnp.bfloat16)
    return (
        mm(grad_b, query, NN),
        mm(prob_b, grad, NN),
        mm(keys_t, grad_b, NN),
    )


def attend(group, dim, blocks, query_all, grad_all, stats, query_t):
    rows = query_all.shape[0]
    cap = rows // group
    for begin in range(0, rows, LANES):
        size = min(LANES, rows - begin)
        part = slice(begin, begin + size)
        query = query_all[part]
        grad = grad_all[part]
        norm, delta = stats[0:1, part], stats[1:2, part]
        total = None
        for keys, keys_t, values, far, diagonal, dkv, first in blocks:
            mask = None
            if diagonal:
                at = begin + lax.broadcasted_iota(jnp.int32, (cap, size), 1)
                at = at - sum(jnp.where(at >= cap * t, cap, 0) for t in range(1, group))
                mask = lax.broadcasted_iota(jnp.int32, (cap, size), 0) <= at
            dk, dv, dq = score_terms(
                keys, keys_t, values, query, grad, norm if far is None else norm + far, delta, mask
            )
            if first and begin == 0:
                dkv[:, :dim] = dk
                dkv[:, dim:] = dv
            else:
                dkv[:, :dim] += dk
                dkv[:, dim:] += dv
            total = dq if total is None else total + dq
        if query_t[1]:
            total = total + query_t[2][:, part]
        query_t[0][:, part] = total


def own_body(group, dim, counts, index, queries, grads, stats, kv, query_t, dkv):
    live = counts[index[0]] * BLOCK
    query_all = stack_heads(queries, group, dim)
    grad_all = stack_heads(grads, group, dim)
    keys, keys_t = masked_keys(kv, dim, live)
    attend(
        group,
        dim,
        [(keys, keys_t, kv[:, dim:], None, True, dkv, True)],
        query_all,
        grad_all,
        stats,
        (query_t, False, None),
    )


def live_of(counts, index, step):
    column, side = index[0] // 2, index[0] % 2
    other = column ^ step
    return jnp.where(other < column, counts[other * 2 + side] * BLOCK, 0)


def far_body(group, dim, steps, counts, index, queries, grads, stats, query_in, *refs):
    kvs, (query_t, *dkvs) = refs[: len(steps)], refs[len(steps) :]
    query_all = stack_heads(queries, group, dim)
    grad_all = stack_heads(grads, group, dim)
    blocks = []
    for step, kv, dkv in zip(steps, kvs, dkvs):
        keys, keys_t = masked_keys(kv, dim, live_of(counts, index, step))
        blocks.append((keys, keys_t, kv[:, dim:], None, False, dkv, True))
    attend(group, dim, blocks, query_all, grad_all, stats, (query_t, True, query_in))


def partner_body(group, dim, steps, counts, index, queries, grads, stats, kv_own, dkv_own, *refs):
    count = len(steps)
    kvs, dkv_in = refs[:count], refs[count : 2 * count]
    query_out, own_out = refs[2 * count], refs[2 * count + 1]
    dkv_out = refs[2 * count + 2 : 3 * count + 2]
    query_t, acc = refs[3 * count + 2], refs[3 * count + 3 :]
    cap = kv_own.shape[0]
    query_all = stack_heads(queries, group, dim)
    grad_all = stack_heads(grads, group, dim)
    keys, keys_t = masked_keys(kv_own, dim, counts[index[0]] * BLOCK)
    hide = jnp.where(index[0] % 2 == 1, FAR, 0.0)
    own_out[...] = dkv_own[...]
    blocks = [(keys, keys_t, kv_own[:, dim:], hide, False, own_out, False)]
    for step, kv, before, total in zip(steps, kvs, dkv_in, acc):
        total[...] = before[...]
        keys, keys_t = masked_keys(kv, dim, live_of(counts, index, step))
        blocks.append((keys, keys_t, kv[:, dim:], None, False, total, False))
    attend(group, dim, blocks, query_all, grad_all, stats, (query_t, False, None))
    for out, total in zip(dkv_out, acc):
        out[...] = total[...].astype(jnp.bfloat16)
    turned = query_t[...].T.astype(jnp.bfloat16)
    for h in range(group):
        query_out[:, h * dim : (h + 1) * dim] = turned[h * cap : (h + 1) * cap]


def sum_body(group, dim, steps, counts, index, query_t, query_in, dkv, *refs):
    count = len(steps)
    incoming = refs[:count]
    rows_out, key_out, value_out = refs[count:]
    cap = query_in.shape[0]
    scale = 1.0 / math.sqrt(dim)
    turned = query_t[...].T
    for h in range(group):
        cols = slice(h * dim, (h + 1) * dim)
        total = turned[h * cap : (h + 1) * cap] + query_in[:, cols].astype(jnp.float32)
        rows_out[:, cols] = (total * scale).astype(jnp.bfloat16)
    column = index[0] // 2
    total = dkv[...]
    for step, part in zip(steps, incoming):
        later = (column ^ step) > column
        total = total + jnp.where(later, part[...].astype(jnp.float32), 0.0)
    rows = lax.broadcasted_iota(jnp.int32, total.shape, 0)
    total = jnp.where(rows < counts[index[0]] * BLOCK, total, 0.0)
    keys, values = total[:, :dim] * scale, total[:, dim:]
    key_out[...] = keys
    value_out[...] = values
    width = group * dim
    rows_out[:, width : width + dim] = keys.astype(jnp.bfloat16)
    rows_out[:, width + dim :] = values.astype(jnp.bfloat16)


def project_body(flip, dtype, head, rows, wq, wk, wv, out):
    width, dim = wq.shape[1], wk.shape[1]
    total = mm(rows[:, :width], wq[...], NT)
    total = total + mm(rows[:, width : width + dim], wk[...], NT)
    total = total + mm(rows[:, width + dim :], wv[...], NT)
    out[...] = total.astype(dtype)


def project(flip, dtype, head, rows, w_query, w_key, w_value, shares):
    cap = rows.shape[0]
    columns = w_query.shape[0] // shares
    tile = math.gcd(columns, 512)
    tiles = columns // tile
    at = lambda t, s: ((s[0] ^ flip) * tiles + t, 0)
    return pl.pallas_call(
        functools.partial(project_body, flip, dtype),
        out_shape=jax.ShapeDtypeStruct((cap, columns), dtype),
        grid_spec=pltpu.PrefetchScalarGridSpec(
            num_scalar_prefetch=1,
            grid=(tiles,),
            in_specs=[
                pl.BlockSpec(rows.shape, lambda t, s: (0, 0)),
                pl.BlockSpec((tile, w_query.shape[1]), at),
                pl.BlockSpec((tile, w_key.shape[1]), at),
                pl.BlockSpec((tile, w_value.shape[1]), at),
            ],
            out_specs=pl.BlockSpec((cap, tile), lambda t, s: (0, t)),
        ),
        name=f"project_{flip}",
    )(head, rows, w_query, w_key, w_value)


def on_device(
    devices,
    shares,
    queries,
    key_states,
    value_states,
    attention_out,
    out_grad,
    log_sum_exp,
    block_counts,
    w_query,
    w_key,
    w_value,
):
    cap, dim = key_states.shape
    group = queries.shape[1] // dim
    rows = cap * group
    columns = devices // 2
    steps = tuple(range(1, columns))
    f32, bf16 = jnp.float32, jnp.bfloat16
    shape = jax.ShapeDtypeStruct
    index = lax.axis_index("ctx").astype(jnp.int32).reshape(1)
    head = lax.axis_index("heads").astype(jnp.int32).reshape(1)

    def swap(x, flip):
        return lax.ppermute(x, "ctx", [(d, d ^ flip) for d in range(devices)])

    def trade(x, flip):
        return lax.ppermute(x, "heads", [(d, d ^ flip) for d in range(shares)])

    queries_p = swap(queries, 1)
    grads_p = swap(out_grad, 1)
    kv = jnp.concatenate([key_states, value_states], axis=1)
    kvs = [swap(kv, 2 * step) for step in steps]
    stats = kernel_call(
        functools.partial(stats_body, group, dim), shape((2, rows), f32), "ssvvv", "stats"
    )(block_counts, index, out_grad, attention_out, log_sum_exp)
    stats_p = swap(stats, 1)
    turned = shape((dim, rows), f32)
    pair = shape((cap, 2 * dim), f32)
    pair_b = shape((cap, 2 * dim), bf16)
    query_t, dkv = kernel_call(
        functools.partial(own_body, group, dim), (turned, pair), "ssvvvv", "own"
    )(block_counts, index, queries, out_grad, stats, kv)
    query_t, *dkvs = kernel_call(
        functools.partial(far_body, group, dim, steps),
        (turned, *[pair] * len(steps)),
        "ss" + "v" * (4 + len(steps)),
        "far",
    )(block_counts, index, queries, out_grad, stats, query_t, *kvs)
    query_p, dkv, *dkvs = pl.pallas_call(
        functools.partial(partner_body, group, dim, steps),
        out_shape=(shape(queries.shape, bf16), pair, *[pair_b] * len(steps)),
        in_specs=[SMEM, SMEM] + [VMEM] * (5 + 2 * len(steps)),
        out_specs=(VMEM,) * (2 + len(steps)),
        scratch_shapes=[pltpu.VMEM((dim, rows), f32)]
        + [pltpu.VMEM((cap, 2 * dim), f32)] * len(steps),
        name="partner",
    )(block_counts, index, queries_p, grads_p, stats_p, kv, dkv, *kvs, *dkvs)
    back = [swap(x, 2 * step) for step, x in zip(steps, dkvs)]
    query_in = swap(query_p, 1)
    flat, key_grad, value_grad = kernel_call(
        functools.partial(sum_body, group, dim, steps),
        (
            shape((cap, queries.shape[1] + 2 * dim), bf16),
            shape((cap, dim), f32),
            shape((cap, dim), f32),
        ),
        "ss" + "v" * (3 + len(steps)),
        "sums",
    )(block_counts, index, query_t, query_in, dkv, *back)

    def reduced(flip, bits):
        if not bits:
            return project(flip, f32, head, flat, w_query, w_key, w_value, shares)
        low = bits[-1]
        away = reduced(flip ^ low, bits[:-1]).astype(bf16)
        sent = trade(away, low)
        return reduced(flip, bits[:-1]) + sent.astype(f32)

    bits = tuple(1 << b for b in range(shares.bit_length() - 1))
    return (reduced(0, bits).astype(bf16), key_grad, value_grad)


def solution(mesh):
    spec = P("ctx", "heads")
    return jax.shard_map(
        functools.partial(on_device, mesh.shape["ctx"], mesh.shape["heads"]),
        mesh=mesh,
        in_specs=(
            spec,
            spec,
            spec,
            spec,
            spec,
            P("heads", "ctx"),
            P(),
            P(None, "heads"),
            P(None, "heads"),
            P(None, "heads"),
        ),
        out_specs=(spec, spec, spec),
        check_vma=False,
    )
```

```python
import functools
import math

import jax
import jax.numpy as jnp
from jax import lax
from jax.experimental import pallas as pl
from jax.experimental.pallas import tpu as pltpu
from jax.sharding import PartitionSpec as P

BLOCK = 64
LOG2E = 1.4426950408889634
FAR = 1e30
LANES = 256
LIMIT = 16 << 20


NT = (((1,), (1,)), ((), ()))
NN = (((1,), (0,)), ((), ()))
VMEM = pl.BlockSpec(memory_space=pltpu.VMEM)
SMEM = pl.BlockSpec(memory_space=pltpu.SMEM)


def mm(a, b, dims):
    return lax.dot_general(a, b, dims, preferred_element_type=jnp.float32)


def kernel_call(body, outs, ins, name, scratch=()):
    call = pl.pallas_call(
        body,
        out_shape=outs,
        in_specs=[SMEM if kind == "s" else VMEM for kind in ins],
        out_specs=jax.tree.map(lambda _: VMEM, outs),
        scratch_shapes=scratch,
        compiler_params=pltpu.CompilerParams(vmem_limit_bytes=LIMIT),
        name=name,
    )
    place = {"s": pltpu.SMEM, "h": pltpu.HBM, "v": pltpu.VMEM}

    def run(*args):
        return call(
            *[pltpu.with_memory_space_constraint(a, place[k]) for a, k in zip(args, ins, strict=True)]
        )

    return run


def stack_heads(ref, group, dim):
    return jnp.concatenate([ref[:, h * dim : (h + 1) * dim] for h in range(group)], axis=0)


def pack_body(dim, counts, index, keys, values, kv):
    rows = lax.broadcasted_iota(jnp.int32, keys.shape, 0)
    live = jnp.where(rows < counts[index[0]] * BLOCK, keys[...].astype(jnp.float32), 0.0)
    kv[:, :dim] = live.astype(jnp.bfloat16)
    kv[:, dim:] = values[...]


def turned_keys(kv, dim):
    return kv[:, :dim].astype(jnp.float32).T.astype(jnp.bfloat16)


def attend(dim, blocks, query_all, grad_all, stats, prob_ref, grad_ref, keys_t):
    rows = query_all.shape[0]
    cap = blocks[0][0].shape[0]
    scale = LOG2E / math.sqrt(dim)
    for number, (kv, far, mask, emit) in enumerate(blocks):
        keys, values = kv[:, :dim], kv[:, dim:]
        here = slice(number * cap, (number + 1) * cap)
        for begin in range(0, rows, LANES):
            size = min(LANES, rows - begin)
            part = slice(begin, begin + size)
            norm, delta = stats[0:1, part], stats[1:2, part]
            if far is not None:
                norm = norm + far
            prob = jnp.exp2(mm(keys, query_all[part], NT) * scale - norm)
            if mask is not None:
                prob = jnp.where(mask(begin, size), prob, 0.0)
            score_grad = prob * (mm(values, grad_all[part], NT) - delta)
            prob_ref[here, part] = prob.astype(jnp.bfloat16)
            grad_ref[here, part] = score_grad.astype(jnp.bfloat16)
        emit(mm(grad_ref[here, :], query_all, NN), mm(prob_ref[here, :], grad_all, NN))
    return mm(keys_t, grad_ref[...], NN)


def own_body(
    group, dim, counts, index, queries, grads, out, norm, kv, stats, query_t, dkv, prob_s, grad_s
):
    cap = grads.shape[0]
    live = counts[index[0]] * BLOCK
    cols = []
    ones = jnp.ones((8, dim), jnp.float32)
    lane = lax.broadcasted_iota(jnp.int32, (1, cap), 1)
    for h in range(group):
        cols_h = slice(h * dim, (h + 1) * dim)
        prod = grads[:, cols_h].astype(jnp.float32) * out[:, cols_h].astype(jnp.float32)
        delta = lax.dot_general(
            ones, prod, NT, precision=lax.Precision.HIGHEST, preferred_element_type=jnp.float32
        )[0:1]
        norm_h = jnp.where(lane < live, norm[h : h + 1, :] * LOG2E, FAR)
        cols.append((norm_h, delta))
    stats[0:1, :] = jnp.concatenate([c[0] for c in cols], axis=1)
    stats[1:2, :] = jnp.concatenate([c[1] for c in cols], axis=1)

    def mask(begin, size):
        at = begin + lax.broadcasted_iota(jnp.int32, (cap, size), 1)
        at = at - sum(jnp.where(at >= cap * t, cap, 0) for t in range(1, group))
        return lax.broadcasted_iota(jnp.int32, (cap, size), 0) <= at

    def emit(dk, dv):
        dkv[:, :dim] = dk
        dkv[:, dim:] = dv

    query_all = stack_heads(queries, group, dim)
    grad_all = stack_heads(grads, group, dim)
    query_t[...] = attend(
        dim, [(kv, None, mask, emit)], query_all, grad_all, stats, prob_s, grad_s, turned_keys(kv, dim)
    )


def hidden(index, step):
    column = index[0] // 2
    return jnp.where((column ^ step) < column, 0.0, FAR)


def far_body(group, dim, steps, index, queries, grads, stats, query_in, *refs):
    count = len(steps)
    kvs, (query_t, *dkvs) = refs[:count], refs[count : 2 * count + 1]
    prob_s, grad_s = refs[2 * count + 1 :]

    def emit_to(out):
        def emit(dk, dv):
            out[:, :dim] = dk
            out[:, dim:] = dv

        return emit

    blocks = [
        (kv, hidden(index, step), None, emit_to(out)) for step, kv, out in zip(steps, kvs, dkvs)
    ]
    keys_t = jnp.concatenate([turned_keys(kv, dim) for kv in kvs], axis=1)
    query_all = stack_heads(queries, group, dim)
    grad_all = stack_heads(grads, group, dim)
    total = attend(dim, blocks, query_all, grad_all, stats, prob_s, grad_s, keys_t)
    query_t[...] = query_in[...] + total


def partner_body(group, dim, steps, index, queries, grads, stats, *refs):
    count = len(steps) + 1
    kvs, before = refs[:count], refs[count : 2 * count]
    query_out, outs = refs[2 * count], refs[2 * count + 1 : 3 * count + 1]
    prob_s, grad_s = refs[3 * count + 1 :]
    cap = kvs[0].shape[0]
    hide = [jnp.where(index[0] % 2 == 1, FAR, 0.0)] + [hidden(index, step) for step in steps]

    def emit_to(start, out):
        def emit(dk, dv):
            out[:, :dim] = (start[:, :dim] + dk).astype(out.dtype)
            out[:, dim:] = (start[:, dim:] + dv).astype(out.dtype)

        return emit

    blocks = [
        (kv, far, None, emit_to(start, out)) for kv, far, start, out in zip(kvs, hide, before, outs)
    ]
    keys_t = jnp.concatenate([turned_keys(kv, dim) for kv in kvs], axis=1)
    query_all = stack_heads(queries, group, dim)
    grad_all = stack_heads(grads, group, dim)
    total = attend(dim, blocks, query_all, grad_all, stats, prob_s, grad_s, keys_t)
    turned = total.T.astype(jnp.bfloat16)
    for h in range(group):
        query_out[:, h * dim : (h + 1) * dim] = turned[h * cap : (h + 1) * cap]


def query_body(group, dim, shares, head, query_t, query_in, w_query, *outs):
    cap = query_in.shape[0]
    scale = 1.0 / math.sqrt(dim)
    turned = query_t[...].T
    parts = []
    for h in range(group):
        total = turned[h * cap : (h + 1) * cap] + query_in[:, h * dim : (h + 1) * dim].astype(
            jnp.float32
        )
        parts.append((total * scale).astype(jnp.bfloat16))
    rows = jnp.concatenate(parts, axis=1)
    project(shares, head, rows, w_query, outs)


def project(shares, head, rows, weight, outs):
    columns = weight.shape[0] // shares
    for flip, out in enumerate(outs):
        at = pl.multiple_of((head[0] ^ flip) * columns, columns)
        out[...] = mm(rows, weight[pl.ds(at, columns), :], NT)


def sum_body(dim, steps, flip, counts, index, head, dkv, wk, wv, before, *refs):
    count = len(steps)
    incoming = refs[:count]
    flat, exact, out = refs[count:]
    scale = 1.0 / math.sqrt(dim)
    column = index[0] // 2
    total = dkv[...]
    for step, part in zip(steps, incoming):
        later = (column ^ step) > column
        total = total + jnp.where(later, part[...].astype(jnp.float32), 0.0)
    rows = lax.broadcasted_iota(jnp.int32, total.shape, 0)
    total = jnp.where(rows < counts[index[0]] * BLOCK, total, 0.0)
    keys, values = total[:, :dim] * scale, total[:, dim:]
    exact[:, :dim] = keys
    exact[:, dim:] = values
    flat[:, :dim] = keys.astype(jnp.bfloat16)
    flat[:, dim:] = values.astype(jnp.bfloat16)
    add_pair(flip, head, flat, wk, wv, before, out)


def add_pair(flip, head, flat, wk, wv, before, out):
    columns, dim = before.shape[1], wk.shape[1]
    at = pl.ds(pl.multiple_of((head[0] ^ flip) * columns, columns), columns)
    total = before[...] + mm(flat[:, :dim], wk[at, :], NT)
    total = total + mm(flat[:, dim:], wv[at, :], NT)
    out[...] = total.astype(out.dtype)


def rest_body(flips, dim, head, flat, exact, wk, wv, *refs):
    count = len(flips)
    key_out, value_out = refs[count : count + 2]
    key_out[...] = exact[:, :dim]
    value_out[...] = exact[:, dim:]
    for flip, before, out in zip(flips, refs[:count], refs[count + 2 :]):
        add_pair(flip, head, flat, wk, wv, before, out)


def on_device(
    devices,
    shares,
    queries,
    key_states,
    value_states,
    attention_out,
    out_grad,
    log_sum_exp,
    block_counts,
    w_query,
    w_key,
    w_value,
):
    cap, dim = key_states.shape
    group = queries.shape[1] // dim
    rows = cap * group
    columns = devices // 2
    steps = tuple(range(1, columns))
    f32, bf16 = jnp.float32, jnp.bfloat16
    shape = jax.ShapeDtypeStruct
    index = lax.axis_index("ctx").astype(jnp.int32).reshape(1)
    head = lax.axis_index("heads").astype(jnp.int32).reshape(1)

    def swap(x, flip):
        return lax.ppermute(x, "ctx", [(d, d ^ flip) for d in range(devices)])

    def trade(x, flip):
        return lax.ppermute(x, "heads", [(d, d ^ flip) for d in range(shares)])

    vmem = pltpu.VMEM
    queries_p = swap(queries, 1)
    grads_p = swap(out_grad, 1)
    kv = kernel_call(
        functools.partial(pack_body, dim), vmem((cap, 2 * dim), bf16), "sshh", "pack"
    )(block_counts, index, key_states, value_states)
    kvs = [swap(kv, 2 * step) for step in reversed(steps)][::-1]
    turned = vmem((dim, rows), f32)
    pair = vmem((cap, 2 * dim), f32)
    pair_b = vmem((cap, 2 * dim), bf16)

    def scratch(count):
        return (vmem((cap * count, rows), bf16),) * 2

    stats, query_t, dkv = kernel_call(
        functools.partial(own_body, group, dim),
        (vmem((2, rows), f32), turned, pair),
        "sshhhhv",
        "own",
        scratch(1),
    )(block_counts, index, queries, out_grad, attention_out, log_sum_exp, kv)
    stats_p = swap(stats, 1)
    query_t, *dkvs = kernel_call(
        functools.partial(far_body, group, dim, steps),
        (turned, *[pair] * len(steps)),
        "shhvv" + "v" * len(steps),
        "far",
        scratch(len(steps)),
    )(index, queries, out_grad, stats, query_t, *kvs)
    query_p, dkv, *dkvs = kernel_call(
        functools.partial(partner_body, group, dim, steps),
        (vmem(queries.shape, bf16), pair, *[pair_b] * len(steps)),
        "svvv" + "v" * (2 * columns),
        "partner",
        scratch(columns),
    )(index, queries_p, grads_p, stats_p, kv, *kvs, dkv, *dkvs)
    query_in = swap(query_p, 1)
    back = [swap(x, 2 * step) for step, x in zip(steps[::-1], dkvs[::-1])][::-1]
    width = w_query.shape[0] // shares
    wide, wide_b = vmem((cap, width), f32), vmem((cap, width), bf16)
    parts = kernel_call(
        functools.partial(query_body, group, dim, shares), (wide,) * shares, "svvv", "query_part"
    )(head, query_t, query_in, w_query)
    last = shares - 1
    small = shape((cap, dim), f32)
    flat, exact, first = kernel_call(
        functools.partial(sum_body, dim, steps, last),
        (pair_b, pair, wide_b),
        "sss" + "v" * (4 + len(steps)),
        "sums",
    )(block_counts, index, head, dkv, w_key, w_value, parts[last], *back)
    flips = tuple(f for f in range(last))
    key_grad, value_grad, *rest = kernel_call(
        functools.partial(rest_body, flips, dim),
        (small, small, *[wide_b if f & 1 else wide for f in flips]),
        "s" + "v" * (4 + len(flips)),
        "rest",
    )(head, flat, exact, w_key, w_value, *parts[:last])
    terms = (*rest, first)

    def reduced(flip, bits):
        if not bits:
            return terms[flip]
        low = bits[-1]
        sent = trade(reduced(flip ^ low, bits[:-1]).astype(bf16), low)
        return reduced(flip, bits[:-1]) + sent.astype(f32)

    bits = tuple(1 << b for b in range(shares.bit_length() - 1))
    return (reduced(0, bits).astype(bf16), key_grad, value_grad)


def solution(mesh):
    spec = P("ctx", "heads")
    return jax.shard_map(
        functools.partial(on_device, mesh.shape["ctx"], mesh.shape["heads"]),
        mesh=mesh,
        in_specs=(
            spec,
            spec,
            spec,
            spec,
            spec,
            P("heads", "ctx"),
            P(),
            P(None, "heads"),
            P(None, "heads"),
            P(None, "heads"),
        ),
        out_specs=(spec, spec, spec),
        check_vma=False,
    )
```

```python
import functools
import math

import jax
import jax.numpy as jnp
from jax import lax
from jax.experimental import pallas as pl
from jax.experimental.pallas import tpu as pltpu
from jax.sharding import PartitionSpec as P

BLOCK = 64
LOG2E = 1.4426950408889634
FAR = 1e30
LANES = 256
LIMIT = 16 << 20


NT = (((1,), (1,)), ((), ()))
NN = (((1,), (0,)), ((), ()))
VMEM = pl.BlockSpec(memory_space=pltpu.VMEM)
SMEM = pl.BlockSpec(memory_space=pltpu.SMEM)
SPECS = {"s": SMEM, "h": VMEM, "v": VMEM, "a": pl.BlockSpec(memory_space=pl.ANY)}


def mm(a, b, dims):
    return lax.dot_general(a, b, dims, preferred_element_type=jnp.float32)


def kernel_call(body, outs, ins, name, scratch=()):
    call = pl.pallas_call(
        body,
        out_shape=outs,
        in_specs=[SPECS[kind] for kind in ins],
        out_specs=jax.tree.map(lambda _: VMEM, outs),
        scratch_shapes=scratch,
        compiler_params=pltpu.CompilerParams(vmem_limit_bytes=LIMIT),
        name=name,
    )
    place = {"s": pltpu.HBM, "h": pltpu.HBM, "v": pltpu.VMEM, "a": pltpu.HBM}

    def run(*args):
        return call(
            *[pltpu.with_memory_space_constraint(a, place[k]) for a, k in zip(args, ins, strict=True)]
        )

    return run


def stack_heads(ref, group, dim):
    return jnp.concatenate([ref[:, h * dim : (h + 1) * dim] for h in range(group)], axis=0)


def place_of():
    return lax.axis_index("ctx").astype(jnp.int32)


def pack_body(dim, counts, keys, values, kv):
    index = place_of()
    rows = lax.broadcasted_iota(jnp.int32, keys.shape, 0)
    live = jnp.where(rows < counts[index] * BLOCK, keys[...].astype(jnp.float32), 0.0)
    kv[:, :dim] = live.astype(jnp.bfloat16)
    kv[:, dim:] = values[...]


def turned_keys(kv, dim):
    return kv[:, :dim].astype(jnp.float32).T.astype(jnp.bfloat16)


def attend(dim, blocks, query_all, grad_all, stats, prob_ref, grad_ref, keys_t):
    rows = query_all.shape[0]
    cap = blocks[0][0].shape[0]
    scale = LOG2E / math.sqrt(dim)
    for number, (kv, far, mask, emit) in enumerate(blocks):
        keys, values = kv[:, :dim], kv[:, dim:]
        here = slice(number * cap, (number + 1) * cap)
        for begin in range(0, rows, LANES):
            size = min(LANES, rows - begin)
            part = slice(begin, begin + size)
            norm, delta = stats[0:1, part], stats[1:2, part]
            if far is not None:
                norm = norm + far
            prob = jnp.exp2(mm(keys, query_all[part], NT) * scale - norm)
            if mask is not None:
                prob = jnp.where(mask(begin, size), prob, 0.0)
            score_grad = prob * (mm(values, grad_all[part], NT) - delta)
            prob_ref[here, part] = prob.astype(jnp.bfloat16)
            grad_ref[here, part] = score_grad.astype(jnp.bfloat16)
        emit(mm(grad_ref[here, :], query_all, NN), mm(prob_ref[here, :], grad_all, NN))
    return mm(keys_t, grad_ref[...], NN)


def own_body(
    group,
    dim,
    counts,
    queries,
    grads,
    out,
    norm,
    kv,
    weight,
    stats,
    query_t,
    dkv,
    weight_out,
    prob_s,
    grad_s,
    sem,
):
    fetch = pltpu.make_async_copy(weight, weight_out, sem)
    fetch.start()
    cap = grads.shape[0]
    index = place_of()
    live = counts[index] * BLOCK
    cols = []
    ones = jnp.ones((8, dim), jnp.float32)
    lane = lax.broadcasted_iota(jnp.int32, (1, cap), 1)
    for h in range(group):
        cols_h = slice(h * dim, (h + 1) * dim)
        prod = grads[:, cols_h].astype(jnp.float32) * out[:, cols_h].astype(jnp.float32)
        delta = lax.dot_general(
            ones, prod, NT, precision=lax.Precision.HIGHEST, preferred_element_type=jnp.float32
        )[0:1]
        norm_h = jnp.where(lane < live, norm[h : h + 1, :] * LOG2E, FAR)
        cols.append((norm_h, delta))
    stats[0:1, :] = jnp.concatenate([c[0] for c in cols], axis=1)
    stats[1:2, :] = jnp.concatenate([c[1] for c in cols], axis=1)

    def mask(begin, size):
        at = begin + lax.broadcasted_iota(jnp.int32, (cap, size), 1)
        at = at - sum(jnp.where(at >= cap * t, cap, 0) for t in range(1, group))
        return lax.broadcasted_iota(jnp.int32, (cap, size), 0) <= at

    def emit(dk, dv):
        dkv[:, :dim] = dk
        dkv[:, dim:] = dv

    query_all = stack_heads(queries, group, dim)
    grad_all = stack_heads(grads, group, dim)
    query_t[...] = attend(
        dim, [(kv, None, mask, emit)], query_all, grad_all, stats, prob_s, grad_s, turned_keys(kv, dim)
    )
    fetch.wait()


def hidden(step):
    column = place_of() // 2
    return jnp.where((column ^ step) < column, 0.0, FAR)


def far_body(group, dim, steps, queries, grads, stats, query_in, *refs):
    count = len(steps)
    kvs, (query_t, *dkvs) = refs[:count], refs[count : 2 * count + 1]
    prob_s, grad_s = refs[2 * count + 1 :]

    def emit_to(out):
        def emit(dk, dv):
            out[:, :dim] = dk
            out[:, dim:] = dv

        return emit

    blocks = [
        (kv, hidden(step), None, emit_to(out)) for step, kv, out in zip(steps, kvs, dkvs)
    ]
    keys_t = jnp.concatenate([turned_keys(kv, dim) for kv in kvs], axis=1)
    query_all = stack_heads(queries, group, dim)
    grad_all = stack_heads(grads, group, dim)
    total = attend(dim, blocks, query_all, grad_all, stats, prob_s, grad_s, keys_t)
    query_t[...] = query_in[...] + total


def partner_body(group, dim, steps, queries, grads, stats, *refs):
    count = len(steps) + 1
    kvs, before = refs[:count], refs[count : 2 * count]
    query_out, outs = refs[2 * count], refs[2 * count + 1 : 3 * count + 1]
    prob_s, grad_s = refs[3 * count + 1 :]
    cap = kvs[0].shape[0]
    hide = [jnp.where(place_of() % 2 == 1, FAR, 0.0)] + [hidden(step) for step in steps]

    def emit_to(start, out):
        def emit(dk, dv):
            out[:, :dim] = (start[:, :dim] + dk).astype(out.dtype)
            out[:, dim:] = (start[:, dim:] + dv).astype(out.dtype)

        return emit

    blocks = [
        (kv, far, None, emit_to(start, out)) for kv, far, start, out in zip(kvs, hide, before, outs)
    ]
    keys_t = jnp.concatenate([turned_keys(kv, dim) for kv in kvs], axis=1)
    query_all = stack_heads(queries, group, dim)
    grad_all = stack_heads(grads, group, dim)
    total = attend(dim, blocks, query_all, grad_all, stats, prob_s, grad_s, keys_t)
    turned = total.T.astype(jnp.bfloat16)
    for h in range(group):
        query_out[:, h * dim : (h + 1) * dim] = turned[h * cap : (h + 1) * cap]


def query_body(group, dim, shares, query_t, query_in, w_query, *outs):
    cap = query_in.shape[0]
    scale = 1.0 / math.sqrt(dim)
    turned = query_t[...].T
    parts = []
    for h in range(group):
        total = turned[h * cap : (h + 1) * cap] + query_in[:, h * dim : (h + 1) * dim].astype(
            jnp.float32
        )
        parts.append((total * scale).astype(jnp.bfloat16))
    rows = jnp.concatenate(parts, axis=1)
    project(shares, rows, w_query, outs)


def project(shares, rows, weight, outs):
    head = lax.axis_index("heads").astype(jnp.int32)
    columns = weight.shape[0] // shares
    for flip, out in enumerate(outs):
        at = pl.multiple_of((head ^ flip) * columns, columns)
        out[...] = mm(rows, weight[pl.ds(at, columns), :], NT)


def sum_body(dim, steps, flip, counts, dkv, wk, wv, before, *refs):
    count = len(steps)
    incoming = refs[:count]
    flat, exact, out = refs[count:]
    scale = 1.0 / math.sqrt(dim)
    index = place_of()
    column = index // 2
    total = dkv[...]
    for step, part in zip(steps, incoming):
        later = (column ^ step) > column
        total = total + jnp.where(later, part[...].astype(jnp.float32), 0.0)
    rows = lax.broadcasted_iota(jnp.int32, total.shape, 0)
    total = jnp.where(rows < counts[index] * BLOCK, total, 0.0)
    keys, values = total[:, :dim] * scale, total[:, dim:]
    exact[:, :dim] = keys
    exact[:, dim:] = values
    flat[:, :dim] = keys.astype(jnp.bfloat16)
    flat[:, dim:] = values.astype(jnp.bfloat16)
    add_pair(flip, flat, wk, wv, before, out)


def add_pair(flip, flat, wk, wv, before, out):
    head = lax.axis_index("heads").astype(jnp.int32)
    columns, dim = before.shape[1], wk.shape[1]
    at = pl.ds(pl.multiple_of((head ^ flip) * columns, columns), columns)
    total = before[...] + mm(flat[:, :dim], wk[at, :], NT)
    total = total + mm(flat[:, dim:], wv[at, :], NT)
    out[...] = total.astype(out.dtype)


def rest_body(flips, dim, flat, exact, wk, wv, *refs):
    count = len(flips)
    key_out, value_out = refs[count : count + 2]
    key_out[...] = exact[:, :dim]
    value_out[...] = exact[:, dim:]
    for flip, before, out in zip(flips, refs[:count], refs[count + 2 :]):
        add_pair(flip, flat, wk, wv, before, out)


def on_device(
    devices,
    shares,
    queries,
    key_states,
    value_states,
    attention_out,
    out_grad,
    log_sum_exp,
    block_counts,
    w_query,
    w_key,
    w_value,
):
    cap, dim = key_states.shape
    group = queries.shape[1] // dim
    rows = cap * group
    columns = devices // 2
    steps = tuple(range(1, columns))
    f32, bf16 = jnp.float32, jnp.bfloat16
    shape = jax.ShapeDtypeStruct
    def swap(x, flip):
        return lax.ppermute(x, "ctx", [(d, d ^ flip) for d in range(devices)])

    def trade(x, flip):
        return lax.ppermute(x, "heads", [(d, d ^ flip) for d in range(shares)])

    vmem = pltpu.VMEM
    kv = kernel_call(
        functools.partial(pack_body, dim), vmem((cap, 2 * dim), bf16), "shh", "pack"
    )(block_counts, key_states, value_states)
    kvs = [swap(kv, 2 * step) for step in reversed(steps)][::-1]
    kv, queries, out_grad = lax.optimization_barrier((kv, queries, out_grad))
    queries_p = swap(queries, 1)
    grads_p = swap(out_grad, 1)
    turned = vmem((dim, rows), f32)
    pair = vmem((cap, 2 * dim), f32)
    pair_b = vmem((cap, 2 * dim), bf16)

    def scratch(count):
        return (vmem((cap * count, rows), bf16),) * 2

    stats, query_t, dkv, w_query = kernel_call(
        functools.partial(own_body, group, dim),
        (vmem((2, rows), f32), turned, pair, vmem(w_query.shape, bf16)),
        "shhhhva",
        "own",
        (*scratch(1), pltpu.SemaphoreType.DMA),
    )(block_counts, queries, out_grad, attention_out, log_sum_exp, kv, w_query)
    stats_p = swap(stats, 1)
    query_t, *dkvs = kernel_call(
        functools.partial(far_body, group, dim, steps),
        (turned, *[pair] * len(steps)),
        "hhvv" + "v" * len(steps),
        "far",
        scratch(len(steps)),
    )(queries, out_grad, stats, query_t, *kvs)
    query_p, dkv, *dkvs = kernel_call(
        functools.partial(partner_body, group, dim, steps),
        (vmem(queries.shape, bf16), pair, *[pair_b] * len(steps)),
        "vvv" + "v" * (2 * columns),
        "partner",
        scratch(columns),
    )(queries_p, grads_p, stats_p, kv, *kvs, dkv, *dkvs)
    query_in = swap(query_p, 1)
    back = [swap(x, 2 * step) for step, x in zip(steps[::-1], dkvs[::-1])][::-1]
    width = w_query.shape[0] // shares
    wide, wide_b = vmem((cap, width), f32), vmem((cap, width), bf16)
    parts = kernel_call(
        functools.partial(query_body, group, dim, shares), (wide,) * shares, "vvv", "query_part"
    )(query_t, query_in, w_query)
    last = shares - 1
    small = shape((cap, dim), f32)
    flat, exact, first = kernel_call(
        functools.partial(sum_body, dim, steps, last),
        (pair_b, pair, wide_b),
        "s" + "v" * (4 + len(steps)),
        "sums",
    )(block_counts, dkv, w_key, w_value, parts[last], *back)
    flips = tuple(f for f in range(last))
    key_grad, value_grad, *rest = kernel_call(
        functools.partial(rest_body, flips, dim),
        (small, small, *[wide_b if f & 1 else wide for f in flips]),
        "v" * (4 + len(flips)),
        "rest",
    )(flat, exact, w_key, w_value, *parts[:last])
    terms = (*rest, first)

    def reduced(flip, bits):
        if not bits:
            return terms[flip]
        low = bits[-1]
        sent = trade(reduced(flip ^ low, bits[:-1]).astype(bf16), low)
        return reduced(flip, bits[:-1]) + sent.astype(f32)

    bits = tuple(1 << b for b in range(shares.bit_length() - 1))
    return (reduced(0, bits).astype(bf16), key_grad, value_grad)


def solution(mesh):
    spec = P("ctx", "heads")
    return jax.shard_map(
        functools.partial(on_device, mesh.shape["ctx"], mesh.shape["heads"]),
        mesh=mesh,
        in_specs=(
            spec,
            spec,
            spec,
            spec,
            spec,
            P("heads", "ctx"),
            P(),
            P(None, "heads"),
            P(None, "heads"),
            P(None, "heads"),
        ),
        out_specs=(spec, spec, spec),
        check_vma=False,
    )
```

```python
import functools
import math

import jax
import jax.numpy as jnp
from jax import lax
from jax.experimental import pallas as pl
from jax.experimental.pallas import tpu as pltpu
from jax.sharding import PartitionSpec as P


BLOCK = 64
LOG2E = 1.4426950408889634
FAR = 1e30
LANES = 256
LIMIT = 16 << 20
CHUNKS = 2


NT = (((1,), (1,)), ((), ()))
NN = (((1,), (0,)), ((), ()))
VMEM = pl.BlockSpec(memory_space=pltpu.VMEM)
SMEM = pl.BlockSpec(memory_space=pltpu.SMEM)
SPECS = {"s": SMEM, "h": VMEM, "v": VMEM, "a": pl.BlockSpec(memory_space=pl.ANY)}


def mm(a, b, dims):
    return lax.dot_general(a, b, dims, preferred_element_type=jnp.float32)


def kernel_call(body, outs, ins, scratch=()):
    call = pl.pallas_call(
        body,
        out_shape=outs,
        in_specs=[SPECS[kind] for kind in ins],
        out_specs=jax.tree.map(lambda _: VMEM, outs),
        scratch_shapes=scratch,
        compiler_params=pltpu.CompilerParams(vmem_limit_bytes=LIMIT),
    )
    place = {"s": pltpu.HBM, "h": pltpu.HBM, "v": pltpu.VMEM, "a": pltpu.HBM}

    def run(*args):
        return call(
            *[
                pltpu.with_memory_space_constraint(a, place[k])
                for a, k in zip(args, ins, strict=True)
            ]
        )

    return run


def stack_heads(ref, group, dim):
    return jnp.concatenate([ref[:, h * dim : (h + 1) * dim] for h in range(group)], axis=0)


def place_of():
    return lax.axis_index("ctx").astype(jnp.int32)


def pack_body(dim, counts, keys, values, kv):
    index = place_of()
    rows = lax.broadcasted_iota(jnp.int32, keys.shape, 0)
    live = jnp.where(rows < counts[index] * BLOCK, keys[...].astype(jnp.float32), 0.0)
    kv[:, :dim] = live.astype(jnp.bfloat16)
    kv[:, dim:] = values[...]


def turned_keys(kv, dim):
    return kv[:, :dim].astype(jnp.float32).T.astype(jnp.bfloat16)


def attend(dim, blocks, query_all, grad_all, stats, prob_ref, grad_ref, keys_t):
    rows = query_all.shape[0]
    cap = blocks[0][0].shape[0]
    scale = LOG2E / math.sqrt(dim)
    for number, (kv, far, mask, emit) in enumerate(blocks):
        keys, values = kv[:, :dim], kv[:, dim:]
        here = slice(number * cap, (number + 1) * cap)
        for begin in range(0, rows, LANES):
            size = min(LANES, rows - begin)
            part = slice(begin, begin + size)
            norm, delta = stats[0:1, part], stats[1:2, part]
            if far is not None:
                norm = norm + far
            prob = jnp.exp2(mm(keys, query_all[part], NT) * scale - norm)
            if mask is not None:
                prob = jnp.where(mask(begin, size), prob, 0.0)
            score_grad = prob * (mm(values, grad_all[part], NT) - delta)
            prob_ref[here, part] = prob.astype(jnp.bfloat16)
            grad_ref[here, part] = score_grad.astype(jnp.bfloat16)
        emit(mm(grad_ref[here, :], query_all[...], NN), mm(prob_ref[here, :], grad_all[...], NN))
    return mm(keys_t, grad_ref[...], NN)


def own_body(
    group,
    dim,
    counts,
    queries,
    grads,
    out,
    norm,
    kv,
    weight,
    stats,
    query_t,
    dkv,
    weight_out,
    query_all,
    grad_all,
    alive,
    prob_s,
    grad_s,
    sem,
):
    fetch = pltpu.make_async_copy(weight, weight_out, sem)
    fetch.start()
    cap = grads.shape[0]
    index = place_of()
    live = counts[index] * BLOCK
    cols = []
    ones = jnp.ones((8, dim), jnp.float32)
    lane = lax.broadcasted_iota(jnp.int32, (1, cap), 1)
    for h in range(group):
        cols_h = slice(h * dim, (h + 1) * dim)
        prod = grads[:, cols_h].astype(jnp.float32) * out[:, cols_h].astype(jnp.float32)
        delta = lax.dot_general(
            ones, prod, NT, precision=lax.Precision.HIGHEST, preferred_element_type=jnp.float32
        )[0:1]
        norm_h = jnp.where(lane < live, norm[h : h + 1, :] * LOG2E, FAR)
        cols.append((norm_h, delta))
    stats[0:1, :] = jnp.concatenate([c[0] for c in cols], axis=1)
    stats[1:2, :] = jnp.concatenate([c[1] for c in cols], axis=1)

    def mask(begin, size):
        at = begin + lax.broadcasted_iota(jnp.int32, (cap, size), 1)
        at = at - sum(jnp.where(at >= cap * t, cap, 0) for t in range(1, group))
        return lax.broadcasted_iota(jnp.int32, (cap, size), 0) <= at

    def emit(dk, dv):
        dkv[:, :dim] = dk
        dkv[:, dim:] = dv

    for h in range(group):
        rows_h, cols_h = slice(h * cap, (h + 1) * cap), slice(h * dim, (h + 1) * dim)
        query_all[rows_h, :] = queries[:, cols_h]
        grad_all[rows_h, :] = grads[:, cols_h]
    rows = lax.broadcasted_iota(jnp.int32, (cap, dim), 0)
    alive[...] = jnp.where(rows < live, 1.0, 0.0)
    query_t[...] = attend(
        dim, [(kv, None, mask, emit)], query_all, grad_all, stats, prob_s, grad_s, turned_keys(kv, dim)
    )
    fetch.wait()


def hidden(step):
    column = place_of() // 2
    return jnp.where((column ^ step) < column, 0.0, FAR)


def far_body(dim, steps, query_all, grad_all, stats, query_in, *refs):
    count = len(steps)
    kvs, (query_t, *dkvs) = refs[:count], refs[count : 2 * count + 1]
    prob_s, grad_s = refs[2 * count + 1 :]

    def emit_to(out):
        def emit(dk, dv):
            out[:, :dim] = dk
            out[:, dim:] = dv

        return emit

    blocks = [
        (kv, hidden(step), None, emit_to(out)) for step, kv, out in zip(steps, kvs, dkvs)
    ]
    keys_t = jnp.concatenate([turned_keys(kv, dim) for kv in kvs], axis=1)
    total = attend(dim, blocks, query_all, grad_all, stats, prob_s, grad_s, keys_t)
    query_t[...] = query_in[...] + total


def chunk_rows(cap):
    count = CHUNKS if cap % (CHUNKS * 16) == 0 else 1
    return [slice(c * cap // count, (c + 1) * cap // count) for c in range(count)]


def partner_body(group, dim, steps, chunks, queries, grads, stats, *refs):
    count = len(steps) + 1
    kvs, before = refs[:count], refs[count : 2 * count]
    query_out, own_out, *refs = refs[2 * count :]
    outs, (prob_s, grad_s) = refs[:-2], refs[-2:]
    cap = kvs[0].shape[0]
    hide = [jnp.where(place_of() % 2 == 1, FAR, 0.0)] + [hidden(step) for step in steps]

    def emit_to(start, pieces):
        def emit(dk, dv):
            for rows, out in pieces:
                out[:, :dim] = (start[rows, :dim] + dk[rows]).astype(out.dtype)
                out[:, dim:] = (start[rows, dim:] + dv[rows]).astype(out.dtype)

        return emit

    pieces = [[(slice(0, cap), own_out)]]
    for at in range(len(steps)):
        pieces.append(list(zip(chunks, outs[at * len(chunks) :])))
    blocks = [
        (kv, far, None, emit_to(start, piece))
        for kv, far, start, piece in zip(kvs, hide, before, pieces)
    ]
    keys_t = jnp.concatenate([turned_keys(kv, dim) for kv in kvs], axis=1)
    query_all = stack_heads(queries, group, dim)
    grad_all = stack_heads(grads, group, dim)
    total = attend(dim, blocks, query_all, grad_all, stats, prob_s, grad_s, keys_t)
    turned = total.T.astype(jnp.bfloat16)
    for h in range(group):
        query_out[:, h * dim : (h + 1) * dim] = turned[h * cap : (h + 1) * cap]


def query_body(group, dim, shares, query_t, query_in, w_query, *outs):
    cap = query_in.shape[0]
    scale = 1.0 / math.sqrt(dim)
    turned = query_t[...].T
    parts = []
    for h in range(group):
        total = turned[h * cap : (h + 1) * cap] + query_in[:, h * dim : (h + 1) * dim].astype(
            jnp.float32
        )
        parts.append((total * scale).astype(jnp.bfloat16))
    rows = jnp.concatenate(parts, axis=1)
    project(shares, rows, w_query, outs)


def project(shares, rows, weight, outs):
    head = lax.axis_index("heads").astype(jnp.int32)
    columns = weight.shape[0] // shares
    for flip, out in enumerate(outs):
        at = pl.multiple_of((head ^ flip) * columns, columns)
        out[...] = mm(rows, weight[pl.ds(at, columns), :], NT)


def sum_body(dim, steps, chunk, flip, alive, dkv, wk, wv, before, *refs):
    count = len(steps)
    incoming = refs[:count]
    flat, exact, out = refs[count:]
    scale = 1.0 / math.sqrt(dim)
    column = place_of() // 2
    total = dkv[chunk, :]
    for step, part in zip(steps, incoming):
        later = (column ^ step) > column
        total = total + jnp.where(later, part[...].astype(jnp.float32), 0.0)
    keep = alive[chunk, :] > 0.0
    keys = jnp.where(keep, total[:, :dim] * scale, 0.0)
    values = jnp.where(keep, total[:, dim:], 0.0)
    exact[:, :dim] = keys
    exact[:, dim:] = values
    flat[:, :dim] = keys.astype(jnp.bfloat16)
    flat[:, dim:] = values.astype(jnp.bfloat16)
    add_pair(flip, chunk, flat, wk, wv, before, out)


def add_pair(flip, chunk, flat, wk, wv, before, out):
    head = lax.axis_index("heads").astype(jnp.int32)
    columns, dim = before.shape[1], wk.shape[1]
    at = pl.ds(pl.multiple_of((head ^ flip) * columns, columns), columns)
    total = before[chunk, :] + mm(flat[:, :dim], wk[at, :], NT)
    total = total + mm(flat[:, dim:], wv[at, :], NT)
    out[...] = total.astype(out.dtype)


def rest_body(flips, chunk, flat, wk, wv, *refs):
    count = len(flips)
    for flip, before, out in zip(flips, refs[:count], refs[count:]):
        add_pair(flip, chunk, flat, wk, wv, before, out)


def last_body(dim, chunks, *refs):
    *ins, input_out, key_out, value_out = refs
    each = len(ins) // len(chunks)
    for at, chunk in enumerate(chunks):
        exact, *terms = ins[at * each : (at + 1) * each]
        key_out[chunk, :] = exact[:, :dim]
        value_out[chunk, :] = exact[:, dim:]
        total = terms[0][...].astype(jnp.float32)
        for term in terms[1:]:
            total = total + term[...].astype(jnp.float32)
        input_out[chunk, :] = total.astype(input_out.dtype)


def on_device(
    devices,
    shares,
    queries,
    key_states,
    value_states,
    attention_out,
    out_grad,
    log_sum_exp,
    block_counts,
    w_query,
    w_key,
    w_value,
):
    cap, dim = key_states.shape
    group = queries.shape[1] // dim
    rows = cap * group
    columns = devices // 2
    steps = tuple(range(1, columns))
    f32, bf16 = jnp.float32, jnp.bfloat16
    shape = jax.ShapeDtypeStruct

    def swap(x, flip):
        return lax.ppermute(x, "ctx", [(d, d ^ flip) for d in range(devices)])

    def trade(x, flip):
        return lax.ppermute(x, "heads", [(d, d ^ flip) for d in range(shares)])

    vmem = pltpu.VMEM
    chunks = chunk_rows(cap)
    kv = kernel_call(functools.partial(pack_body, dim), vmem((cap, 2 * dim), bf16), "shh")(
        block_counts, key_states, value_states
    )
    kvs = [swap(kv, 2 * step) for step in steps]
    queries_p = swap(queries, 1)
    grads_p = swap(out_grad, 1)
    turned = vmem((dim, rows), f32)
    pair = vmem((cap, 2 * dim), f32)

    def scratch(count):
        return (vmem((cap * count, rows), bf16),) * 2

    stats, query_t, dkv, w_query, query_all, grad_all, alive = kernel_call(
        functools.partial(own_body, group, dim),
        (
            vmem((2, rows), f32),
            turned,
            pair,
            vmem(w_query.shape, bf16),
            vmem((rows, dim), bf16),
            vmem((rows, dim), bf16),
            vmem((cap, dim), f32),
        ),
        "shhhhva",
        (*scratch(1), pltpu.SemaphoreType.DMA),
    )(block_counts, queries, out_grad, attention_out, log_sum_exp, kv, w_query)
    stats_p = swap(stats, 1)
    query_t, *dkvs = kernel_call(
        functools.partial(far_body, dim, steps),
        (turned, *[pair] * len(steps)),
        "vvvv" + "v" * len(steps),
        scratch(len(steps)),
    )(query_all, grad_all, stats, query_t, *kvs)
    size = cap // len(chunks)
    query_p, dkv, *dkvs = kernel_call(
        functools.partial(partner_body, group, dim, steps, chunks),
        (vmem(queries.shape, bf16), pair)
        + (vmem((size, 2 * dim), bf16),) * (len(steps) * len(chunks)),
        "vvv" + "v" * (2 * columns),
        scratch(columns),
    )(queries_p, grads_p, stats_p, kv, *kvs, dkv, *dkvs)
    query_in = swap(query_p, 1)
    back = [
        [swap(dkvs[at * len(chunks) + c], 2 * step) for at, step in enumerate(steps)]
        for c in range(len(chunks))
    ]
    width = w_query.shape[0] // shares
    wide = vmem((cap, width), f32)
    parts = kernel_call(
        functools.partial(query_body, group, dim, shares), (wide,) * shares, "vvv"
    )(query_t, query_in, w_query)
    top = shares - 1
    flips = tuple(range(top))
    bits = tuple(1 << b for b in range(shares.bit_length() - 1))
    some, some_b = vmem((size, width), f32), vmem((size, width), bf16)
    ends = []
    for c, chunk in enumerate(chunks):
        flat, exact, first = kernel_call(
            functools.partial(sum_body, dim, steps, chunk, top),
            (vmem((size, 2 * dim), bf16), vmem((size, 2 * dim), f32), some_b),
            "v" * (5 + len(steps)),
        )(alive, dkv, w_key, w_value, parts[top], *back[c])
        rest = kernel_call(
            functools.partial(rest_body, flips, chunk),
            tuple(some_b if f & 1 else some for f in flips),
            "v" * (3 + len(flips)),
        )(flat, w_key, w_value, *parts[:top])
        terms = (*rest, first)

        def arrivals(flip, bits):
            return [trade(reduced(flip ^ bit, bits[:at]), bit) for at, bit in enumerate(bits)]

        def reduced(flip, bits):
            total = terms[flip].astype(f32)
            for part in arrivals(flip, bits):
                total = total + part.astype(f32)
            return total.astype(bf16)

        ends += [exact, terms[0], *arrivals(0, bits)]
    return kernel_call(
        functools.partial(last_body, dim, chunks),
        (shape((cap, width), bf16), shape((cap, dim), f32), shape((cap, dim), f32)),
        "v" * len(ends),
    )(*ends)


def solution(mesh):
    spec = P("ctx", "heads")
    devices, shares = mesh.shape["ctx"], mesh.shape["heads"]

    def body(*args):
        return on_device(devices, shares, *args)

    return jax.shard_map(
        body,
        mesh=mesh,
        in_specs=(
            spec,
            spec,
            spec,
            spec,
            spec,
            P("heads", "ctx"),
            P(),
            P(None, "heads"),
            P(None, "heads"),
            P(None, "heads"),
        ),
        out_specs=(spec, spec, spec),
        check_vma=False,
    )
```
